32 devices in a mesh: dp: 8 (over z, core), mp: 4 (over y, x).
Axes of the slice: x: 2, y: 2, z: 4, core: 2. Of those that a mesh axis runs over, the one named last changes fastest.
Arguments:
- features: bfloat16 [8192, 8192], P('dp', 'mp'), may hold values from -6 to 6
- v_weight: bfloat16 [3, 8192, 1024], P(None, 'mp', 'dp'), may hold values from -0.0625 to 0.0625
- u_weight: bfloat16 [3, 1024, 8192], P(None, 'dp', 'mp'), may hold values from -0.1875 to 0.1875
- cross_bias: float32 [3, 8192], P(None, 'mp'), may hold values from -3 to 3
Outputs:
- crossed: bfloat16 [8192, 8192], P('dp', 'mp')
The draws below stay inside these ranges and needn't reach their ends.
All inputs are finite; a program needn't handle non-finite values.
Results may differ from the reference program's by a relative error of at most 0.009.
Values may be sent and summed in bfloat16 or wider, within the bound.
No kernel may reach another device: no remote copies, remote signals or barrier semaphores. Data moves between devices by JAX's collectives and lax.ppermute only.
A program may use at most 128 MiB of HBM per device.

```python
import jax
import jax.numpy as jnp

D = 8192
R = 1024
LAYERS = 3
BATCH = 8192


def block_levels(key, extent, split, low, top_value):
    factor_of = 1.0
    for axis_at, blocks in split:
        draws = jax.random.uniform(jax.random.fold_in(jax.random.fold_in(key, 6), axis_at), (blocks,), jnp.float32, low / len(split), top_value / len(split))
        factor_of = factor_of * jnp.repeat(jnp.exp(draws), extent[axis_at] // blocks).reshape((-1,) + (1,) * (len(extent) - 1 - axis_at))
    return factor_of


def scatter_about(key, shape, width, reach, shards=(), kind=jnp.bfloat16):
    entries = jax.random.normal(key, shape, jnp.float32) * width
    if len(shards) > 0:
        entries = block_levels(key, shape, shards, -0.22, 0.18) * entries
    return jnp.clip(entries, min=-reach, max=reach).astype(kind)


def setup_inputs(seed: int = 0) -> dict:
    key_of = jax.random.split(jax.random.key(seed), 5)
    features = scatter_about(key_of[0], (BATCH, D), 1.0, 6.0, ((0, 8), (1, 4)))
    v_weight = scatter_about(key_of[1], (LAYERS, D, R), D ** -0.5, 0.0625, ((1, 4), (2, 8)))
    u_weight = scatter_about(key_of[2], (LAYERS, R, D), R ** -0.5, 0.1875, ((1, 8), (2, 4)))
    cross_bias = scatter_about(key_of[3], (LAYERS, D), 0.5, 3.0, ((1, 4),), jnp.float32)
    return {"features": features, "v_weight": v_weight, "u_weight": u_weight, "cross_bias": cross_bias}


def reference(features, v_weight, u_weight, cross_bias):
    carried = features
    for layer_number in range(LAYERS):
        rank_proj = jnp.dot(carried, v_weight[layer_number], preferred_element_type=jnp.float32).astype(jnp.bfloat16)
        cross_term = jnp.dot(rank_proj, u_weight[layer_number], preferred_element_type=jnp.float32) + cross_bias[layer_number]
        carried = (features.astype(jnp.float32) * cross_term + carried.astype(jnp.float32)).astype(jnp.bfloat16)
    return carried
```

```python
import functools

import jax
import jax.numpy as jnp
from jax import lax
from jax.sharding import PartitionSpec as P


def swap(value, bit, size):
    return lax.ppermute(value, "mp", [(i, i ^ bit) for i in range(size)])


def sum_over_mp(partial_value, bits, size):
    position = lax.axis_index("mp")
    mine = partial_value
    for bit in bits:
        rows = mine.shape[0] // 2
        low, high = mine[:rows], mine[rows:]
        upper = (position & bit) != 0
        sent = jnp.where(upper, low, high).astype(jnp.bfloat16)
        kept = jnp.where(upper, high, low)
        mine = kept + swap(sent, bit, size).astype(jnp.float32)
    mine = mine.astype(jnp.bfloat16)
    for bit in reversed(bits):
        other = swap(mine, bit, size)
        upper = (position & bit) != 0
        mine = jnp.concatenate(
            [jnp.where(upper, other, mine), jnp.where(upper, mine, other)], axis=0
        )
    return mine


def local(features, v_weight, u_weight, cross_bias, *, mp, chunks):
    layers = v_weight.shape[0]
    bits = [1 << k for k in range(mp.bit_length() - 1)]
    rows = features.shape[0] // chunks
    base = [features[c * rows : (c + 1) * rows] for c in range(chunks)]
    carried = list(base)
    for layer_number in range(layers):
        v_full = lax.all_gather(v_weight[layer_number], "dp", axis=1, tiled=True)
        u_full = lax.all_gather(u_weight[layer_number], "dp", axis=0, tiled=True)
        for c in range(chunks):
            current = carried[c]
            partial_value = jnp.dot(current, v_full, preferred_element_type=jnp.float32)
            order = bits if c % 2 == 0 else bits[::-1]
            rank_proj = sum_over_mp(partial_value, order, mp)
            cross_term = jnp.dot(rank_proj, u_full, preferred_element_type=jnp.float32)
            cross_term = cross_term + cross_bias[layer_number]
            carried[c] = (
                base[c].astype(jnp.float32) * cross_term + current.astype(jnp.float32)
            ).astype(jnp.bfloat16)
    return jnp.concatenate(carried, axis=0)


def solution(mesh):
    return jax.shard_map(
        functools.partial(local, mp=mesh.shape["mp"], chunks=2),
        mesh=mesh,
        in_specs=(P("dp", "mp"), P(None, "mp", "dp"), P(None, "dp", "mp"), P(None, "mp")),
        out_specs=P("dp", "mp"),
        check_vma=False,
    )
```

```python
import functools

import jax
import jax.numpy as jnp
from jax import lax
from jax.sharding import PartitionSpec as P

RELAY = True
PERMUTED_LAYERS = (1,)


def swap(value, bit, size):
    return lax.ppermute(value, "mp", [(i, i ^ bit) for i in range(size)])


def sum_over_mp(partial_value, bits, size):
    position = lax.axis_index("mp")
    mine = partial_value
    for bit in bits:
        rows = mine.shape[0] // 2
        low, high = mine[:rows], mine[rows:]
        upper = (position & bit) != 0
        sent = jnp.where(upper, low, high).astype(jnp.bfloat16)
        kept = jnp.where(upper, high, low)
        mine = kept + swap(sent, bit, size).astype(jnp.float32)
    mine = mine.astype(jnp.bfloat16)
    for bit in reversed(bits):
        other = swap(mine, bit, size)
        upper = (position & bit) != 0
        mine = jnp.concatenate(
            [jnp.where(upper, other, mine), jnp.where(upper, mine, other)], axis=0
        )
    return mine


def collect_over_dp(value, size):
    cores = 2 if size % 2 == 0 else 1
    chips = size // cores
    place = lax.axis_index("dp") // cores

    def shift(piece, step, wrap):
        pairs = []
        for i in range(size):
            to = i + step * cores
            if wrap or 0 <= to < size:
                pairs.append((i, to % size))
        return lax.ppermute(piece, "dp", pairs)

    slots = {0: value}
    for step in (1, chips - 1) if RELAY else range(1, chips):
        if step not in slots:
            slots[step] = shift(value, step, True)
    if RELAY and chips > 3:
        up, down = {1: slots[1]}, {1: slots[chips - 1]}
        for step in range(2, chips - 1):
            up[step] = shift(up[step - 1], 1, False)
            down[step] = shift(down[step - 1], -1, False)
        for step in range(2, chips - 1):
            slots[step] = jnp.where(place >= step, up[step], down[chips - step])
    mine = jnp.concatenate([slots[step] for step in range(chips)], axis=0)
    if cores == 1:
        return mine
    other = lax.ppermute(mine, "dp", [(i, i ^ 1) for i in range(size)])
    return jnp.concatenate([mine, other], axis=0)


def local(features, v_weight, u_weight, cross_bias, *, dp, mp, chunks):
    layers = v_weight.shape[0]
    bits = [1 << k for k in range(mp.bit_length() - 1)]
    rows = features.shape[0] // chunks
    base = [features[c * rows : (c + 1) * rows] for c in range(chunks)]
    carried = list(base)
    for layer_number in range(layers):
        if layer_number in PERMUTED_LAYERS:
            v_full = collect_over_dp(v_weight[layer_number].T, dp)
            u_full = collect_over_dp(u_weight[layer_number], dp)
            v_contract = 1
        else:
            v_full = lax.all_gather(v_weight[layer_number], "dp", axis=1, tiled=True)
            u_full = lax.all_gather(u_weight[layer_number], "dp", axis=0, tiled=True)
            v_contract = 0
        for c in range(chunks):
            current = carried[c]
            partial_value = lax.dot_general(current, v_full, (((1,), (v_contract,)), ((), ())), preferred_element_type=jnp.float32)
            order = bits if c % 2 == 0 else bits[::-1]
            rank_proj = sum_over_mp(partial_value, order, mp)
            cross_term = jnp.dot(rank_proj, u_full, preferred_element_type=jnp.float32)
            cross_term = cross_term + cross_bias[layer_number]
            carried[c] = (
                base[c].astype(jnp.float32) * cross_term + current.astype(jnp.float32)
            ).astype(jnp.bfloat16)
    return jnp.concatenate(carried, axis=0)


def solution(mesh):
    return jax.shard_map(
        functools.partial(local, dp=mesh.shape["dp"], mp=mesh.shape["mp"], chunks=2),
        mesh=mesh,
        in_specs=(P("dp", "mp"), P(None, "mp", "dp"), P(None, "dp", "mp"), P(None, "mp")),
        out_specs=P("dp", "mp"),
        check_vma=False,
    )
```
